32 devices in a mesh: row: 4 (over z), col: 4 (over x, core), img: 2 (over y).
Axes of the slice: x: 2, y: 2, z: 4, core: 2. Of those that a mesh axis runs over, the one named last changes fastest.
Arguments:
- tokens: bfloat16 [96, 144, 512], P(('img', 'row'), 'col'), parts along dimension 0, may hold values from -6 to 6
- qkv_weight: bfloat16 [2, 512, 1536], P(None, 'col'), may hold values from -0.25 to 0.25
- proj_weight: bfloat16 [2, 512, 512], P(None, 'col'), may hold values from -0.25 to 0.25
- hidden_weight: bfloat16 [2, 512, 2048], P(None, 'col'), may hold values from -0.25 to 0.25
- output_weight: bfloat16 [2, 2048, 512], P(None, 'col'), may hold values from -0.125 to 0.125
- norm_gain: float32 [2, 2, 512], replicated, may hold values from 0.25 to 1.75
- model_bias: float32 [2, 4, 512], replicated, may hold values from -2 to 2
- qkv_bias: float32 [2, 1536], replicated, may hold values from -2 to 2
- hidden_bias: float32 [2, 2048], replicated, may hold values from -2 to 2
- position_bias: float32 [2, 16, 23, 23], replicated, may hold values from -3 to 250
Outputs:
- result: bfloat16 [96, 144, 512], P(('img', 'row'), 'col'), parts along dimension 0
The draws below stay inside these ranges and needn't reach their ends.
There are 2 independent parts, one for each index of `img`. The reference program is written for one: setup_inputs(seed, part) draws one part's arguments, and reference() takes and returns one part's arrays. A program takes and returns all parts, laid end to end along the dimension named above; an argument that names none is the same for every part. Nothing has to cross between parts.
All inputs are finite; a program needn't handle non-finite values.
Results may differ from the reference program's by a relative error of at most 0.012.
Values may be sent and summed in bfloat16 or wider, within the bound.
A program may use at most 192 MiB of HBM per device.

```python
import jax
import jax.numpy as jnp
from jax import lax

D = 512
HEADS = 16
FF = 2048
WIN = 12
BLOCKS = 2
SHIFT = 6
H = 48
W = 144


def draw_position_bias(key, part):
    values = jnp.clip(jax.random.normal(key, (BLOCKS, HEADS, 2 * WIN - 1, 2 * WIN - 1), jnp.float32), -3.0, 3.0)
    return values


def steps_of(key, shape, cuts, smallest, largest):
    loudness = 1.0
    for dim, shards_of in cuts:
        heights = jax.random.uniform(jax.random.fold_in(jax.random.fold_in(key, 6), dim), (shards_of,), jnp.float32, smallest / len(cuts), largest / len(cuts))
        loudness = loudness * jnp.repeat(jnp.exp(heights), shape[dim] // shards_of).reshape((-1,) + (1,) * (len(shape) - 1 - dim))
    return loudness


def bell_draw(stream_key, extent, scale, limit, cuts=(), kind=jnp.bfloat16):
    drawn = scale * jax.random.normal(stream_key, extent, jnp.float32)
    if cuts:
        drawn = drawn * steps_of(stream_key, extent, cuts, -0.22, 0.18)
    return jnp.clip(drawn, -limit, limit).astype(kind)


def setup_inputs(seed: int = 0, part: int = 0) -> dict:
    key_list = jax.random.split(jax.random.key(seed), 11)
    own_keys = jax.random.split(jax.random.fold_in(key_list[10], part), 11)
    tokens = bell_draw(own_keys[0], (H, W, D), 1.0, 6.0, ((0, 4), (1, 4)))
    qkv_weight = bell_draw(key_list[1], (BLOCKS, D, 3 * D), D ** -0.5, 0.25, ((1, 4),))
    proj_weight = bell_draw(key_list[2], (BLOCKS, D, D), D ** -0.5, 0.25, ((1, 4),))
    hidden_weight = bell_draw(key_list[3], (BLOCKS, D, FF), D ** -0.5, 0.25, ((1, 4),))
    output_weight = bell_draw(key_list[4], (BLOCKS, FF, D), FF ** -0.5, 0.125, ((1, 4),))
    norm_gain = jnp.clip(1.0 + 0.15 * jax.random.normal(key_list[5], (BLOCKS, 2, D), jnp.float32), 0.25, 1.75)
    model_bias = bell_draw(key_list[6], (BLOCKS, 4, D), 0.3, 2.0, (), jnp.float32)
    qkv_bias = bell_draw(key_list[7], (BLOCKS, 3 * D), 0.3, 2.0, (), jnp.float32)
    hidden_bias = bell_draw(key_list[8], (BLOCKS, FF), 0.3, 2.0, (), jnp.float32)
    position_bias = draw_position_bias(jax.random.fold_in(key_list[10], 71), part)
    return dict(tokens=tokens, qkv_weight=qkv_weight, proj_weight=proj_weight, hidden_weight=hidden_weight, output_weight=output_weight, norm_gain=norm_gain, model_bias=model_bias, qkv_bias=qkv_bias, hidden_bias=hidden_bias, position_bias=position_bias)


def layer_norm(values, gain, shift):
    center = values - lax.optimization_barrier(jnp.mean(values, -1, keepdims=True))
    spread = lax.optimization_barrier(jnp.mean(center * center, -1, keepdims=True))
    return center * lax.rsqrt(spread + 1e-05) * gain + shift

def bias_table(table):
    offsets = jnp.arange(WIN)
    delta = (offsets[:, None] - offsets[None, :] + WIN - 1).astype(jnp.int32)
    picked = table[:, delta[:, None, :, None], delta[None, :, None, :]]
    return picked.reshape(table.shape[0], WIN * WIN, WIN * WIN)

def labels(start, count, total):
    index = start + jnp.arange(count)
    return (index >= total - WIN).astype(jnp.int32) + (index >= total - SHIFT).astype(jnp.int32)

def window_attention(qkv_band, position, label_grid):
    width = qkv_band.shape[1]
    nwin = width // WIN
    head_dim = D // HEADS
    split = qkv_band.reshape(WIN, nwin, WIN, 3, HEADS, head_dim).transpose(1, 0, 2, 3, 4, 5)
    split = split.reshape(nwin, WIN * WIN, 3, HEADS, head_dim)
    query = split[:, :, 0].astype(jnp.float32)
    keys = split[:, :, 1].astype(jnp.float32)
    values = split[:, :, 2].astype(jnp.float32)
    scores = jnp.einsum('wqhd,wkhd->whqk', query, keys) / jnp.sqrt(jnp.float32(head_dim)) + position[None]
    if label_grid is not None:
        window_labels = label_grid.reshape(WIN, nwin, WIN).transpose(1, 0, 2).reshape(nwin, WIN * WIN)
        same = window_labels[:, :, None] == window_labels[:, None, :]
        scores = jnp.where(same[:, None], scores, -1000000000.0)
    attn = jax.nn.softmax(scores, -1).astype(jnp.bfloat16)
    heads_out = jnp.einsum('whqk,wkhd->wqhd', attn.astype(jnp.float32), values).astype(jnp.bfloat16)
    return heads_out.reshape(nwin, WIN, WIN, D).transpose(1, 0, 2, 3).reshape(WIN, width, D)

def swin_block(grid, layer, masked, qkv_weight, proj_weight, hidden_weight, output_weight, norm_gain, model_bias, qkv_bias, hidden_bias, position_bias):
    height, width = (grid.shape[0], grid.shape[1])
    flat = grid.reshape(-1, D).astype(jnp.float32)
    normed = layer_norm(flat, norm_gain[layer, 0], model_bias[layer, 0]).astype(jnp.bfloat16)
    qkv = (jnp.dot(normed, qkv_weight[layer], preferred_element_type=jnp.float32) + qkv_bias[layer]).astype(jnp.bfloat16)
    qkv = qkv.reshape(height, width, 3 * D)
    position = bias_table(position_bias[layer])
    column_labels = labels(0, width, width)

    def one_band(band):
        start = (band * WIN).astype(jnp.int32)
        rows_here = lax.dynamic_slice_in_dim(qkv, start, WIN, 0)
        if masked:
            grid_labels = labels(start, WIN, height)[:, None] * 3 + column_labels[None, :]
        else:
            grid_labels = None
        return window_attention(rows_here, position, grid_labels)
    heads_out = lax.map(one_band, jnp.arange(height // WIN).astype(jnp.int32)).reshape(-1, D)
    middle = flat + (jnp.dot(heads_out, proj_weight[layer], preferred_element_type=jnp.float32) + model_bias[layer, 2])
    normed2 = layer_norm(middle, norm_gain[layer, 1], model_bias[layer, 1]).astype(jnp.bfloat16)
    hidden = jax.nn.gelu(jnp.dot(normed2, hidden_weight[layer], preferred_element_type=jnp.float32) + hidden_bias[layer], approximate=False).astype(jnp.bfloat16)
    final = middle + (jnp.dot(hidden, output_weight[layer], preferred_element_type=jnp.float32) + model_bias[layer, 3])
    return final.astype(jnp.bfloat16).reshape(height, width, D)

def reference(tokens, qkv_weight, proj_weight, hidden_weight, output_weight, norm_gain, model_bias, qkv_bias, hidden_bias, position_bias):
    params = (qkv_weight, proj_weight, hidden_weight, output_weight, norm_gain, model_bias, qkv_bias, hidden_bias, position_bias)
    first = swin_block(tokens, 0, False, *params)
    shifted = jnp.roll(first, (-SHIFT, -SHIFT), (0, 1))
    second = swin_block(shifted, 1, True, *params)
    return jnp.roll(second, (SHIFT, SHIFT), (0, 1))
```

```python
import functools

import jax
import jax.numpy as jnp
import numpy as np
from jax import lax
from jax.experimental import pallas as pl
from jax.experimental.pallas import tpu as pltpu
from jax.sharding import PartitionSpec as P

HEADS = 16
WIN = 12
SHIFT = 6
HALF = WIN // 2
PATCH = HALF * HALF
AREA = WIN * WIN
GROUP = 4
LOG2E = 1.4426950408889634
MESH = pl.DeviceIdType.MESH


def position_tables(table):
    layers, heads = table.shape[:2]
    coord = np.arange(WIN)
    onehot = (coord[None, :, None] - coord[:, None, None] + WIN - 1 == np.arange(2 * WIN - 1)).astype(np.float32)
    rows = jnp.einsum("kqa,lhab->lhkqb", onehot, table, precision=lax.Precision.HIGHEST)
    both = jnp.einsum("lhkqb,xyb->lhkqxy", rows, onehot, precision=lax.Precision.HIGHEST)
    both = both * LOG2E
    both = both.reshape(layers, heads // GROUP, GROUP, 2, HALF, 2, HALF, 2, HALF, 2, HALF)
    both = both.transpose(0, 1, 3, 7, 4, 8, 2, 5, 9, 6, 10)
    return both.reshape(layers, heads // GROUP, AREA, GROUP * AREA)


def layer_norm(values, gain, shift):
    center = values - jnp.mean(values, -1, keepdims=True)
    spread = jnp.mean(center * center, -1, keepdims=True)
    return center * lax.rsqrt(spread + 1e-05) * gain + shift


def kernel(
    sizes,
    tokens_hbm, qkv_hbm, proj_hbm, hid_hbm, outw_hbm,
    gain_ref, mbias_ref, qkvb_ref, hidb_ref, pos_hbm,
    out_ref,
    wqkv, wproj, whid, wout, pos_ref, tok_ref, tok32, x32, normed, qkv_ref, heads_ref, hidden_ref, y32,
    stage, rowdiff, coldiff,
    sa, sb, sc, ra, rb, rc,
    local_sem, psend, precv, xsend, xrecv, ysend, yrecv, fsend, frecv, hsend, hrecv,
):
    n_row, n_col, n_img = sizes
    chips = n_col // 2
    row, col, img = lax.axis_index("row"), lax.axis_index("col"), lax.axis_index("img")
    chip, core = col // 2, col % 2
    channels = x32.shape[1]
    nwin = x32.shape[0] // AREA
    ncols = 2 * nwin
    partner = {"col": chip * 2 + (1 - core)}
    ypeer = {"img": (img + 1) % n_img}

    def xpeer(t):
        return {"col": lax.rem(chip + t, chips) * 2 + core}

    up, down = lax.rem(row + n_row - 1, n_row), lax.rem(row + 1, n_row)
    left, right = lax.rem(col + n_col - 1, n_col), lax.rem(col + 1, n_col)
    back = ({"row": up}, {"col": left}, {"row": up, "col": left})
    forth = ({"row": down}, {"col": right}, {"row": down, "col": right})

    barrier = pltpu.get_barrier_semaphore()
    greet = [partner, ypeer, *(xpeer(t) for t in range(1, chips)), *back, *forth]
    for target in greet:
        pl.semaphore_signal(barrier, inc=1, device_id=target, device_id_type=MESH)
    tok_copy = pltpu.make_async_copy(tokens_hbm, tok_ref, local_sem.at[8])
    tok_copy.start()
    pl.semaphore_wait(barrier, len(greet))

    hbm = (qkv_hbm, proj_hbm, hid_hbm, outw_hbm)
    vmem = (wqkv, wproj, whid, wout)
    halves = n_img

    def shard(kind, layer, owner):
        rows = hbm[kind].shape[1]
        return vmem[kind].at[layer, pl.ds(pl.multiple_of(owner * rows, rows), rows), :]

    def part(kind, layer, owner, half):
        rows = hbm[kind].shape[1]
        size = rows // halves
        return vmem[kind].at[layer, pl.ds(pl.multiple_of(owner * rows + half * size, size), size), :]

    def remote(src, dst, send, recv, target):
        return pltpu.make_async_remote_copy(
            src_ref=src, dst_ref=dst, send_sem=send, recv_sem=recv, device_id=target, device_id_type=MESH
        )

    sends = []
    for t in range(8):
        layer, kind = divmod(t, 4)
        rows = hbm[kind].shape[1]
        size = rows // halves
        mine = hbm[kind].at[layer, pl.ds(pl.multiple_of(img * size, size), size), :]
        for d in range(1, chips):
            copy = remote(mine, part(kind, layer, col, img), xsend.at[t, d - 1], xrecv.at[t, d - 1], xpeer(d))
            copy.start()
            sends.append(copy)
        copy = remote(hbm[kind].at[layer], shard(kind, layer, col), psend.at[t], precv.at[t], partner)
        copy.start()
        sends.append(copy)
        pltpu.make_async_copy(hbm[kind].at[layer], shard(kind, layer, col), local_sem.at[t]).start()
        if t == 0:
            pos_copy = pltpu.make_async_copy(pos_hbm, pos_ref, local_sem.at[9])
            pos_copy.start()

    def owner_at(d, lane):
        return lax.rem(chip + chips - d, chips) * 2 + lane

    def forward_x(t):
        layer, kind = divmod(t, 4)
        for d in range(1, chips):
            got = part(kind, layer, owner_at(d, core), img)
            remote(got, got, xsend.at[t, d - 1], xrecv.at[t, d - 1], xpeer(d)).wait_recv()
            for copy in (
                remote(got, got, ysend.at[t, d - 1], yrecv.at[t, d - 1], ypeer),
                remote(got, got, fsend.at[t, d - 1, 0], frecv.at[t, d - 1, 0], partner),
            ):
                copy.start()
                sends.append(copy)

    def forward_y(t):
        layer, kind = divmod(t, 4)
        for d in range(1, chips):
            got = part(kind, layer, owner_at(d, core), 1 - img)
            remote(got, got, ysend.at[t, d - 1], yrecv.at[t, d - 1], ypeer).wait_recv()
            copy = remote(got, got, fsend.at[t, d - 1, 1], frecv.at[t, d - 1, 1], partner)
            copy.start()
            sends.append(copy)

    def ready(t):
        layer, kind = divmod(t, 4)
        pltpu.make_async_copy(hbm[kind].at[layer], shard(kind, layer, col), local_sem.at[t]).wait()
        other = shard(kind, layer, chip * 2 + (1 - core))
        remote(other, other, psend.at[t], precv.at[t], partner).wait_recv()
        for d in range(1, chips):
            for k, half in ((0, img), (1, 1 - img)):
                got = part(kind, layer, owner_at(d, 1 - core), half)
                remote(got, got, fsend.at[t, d - 1, k], frecv.at[t, d - 1, k], partner).wait_recv()

    def iota(shape, dim):
        return lax.broadcasted_iota(jnp.int32, shape, dim)

    wide = GROUP * AREA
    key = iota((AREA, wide), 0)
    query = iota((AREA, wide), 1) % AREA
    rowdiff[...] = ((key // (2 * PATCH)) != (query // (2 * PATCH))).astype(jnp.float32)
    coldiff[...] = (((key // PATCH) % 2) != ((query // PATCH) % 2)).astype(jnp.float32)
    pick = (key == query).astype(jnp.bfloat16)
    head_dim = channels // HEADS
    lanes = GROUP * head_dim
    own_head = iota((lanes, wide), 0) // head_dim == iota((lanes, wide), 1) // AREA
    head_masks = [(iota((AREA, lanes), 1) // head_dim == h).astype(jnp.bfloat16) for h in range(GROUP)]
    last_row = (row == n_row - 1).astype(jnp.float32)
    last_col = (col == n_col - 1).astype(jnp.float32)

    def base(half, patch_col):
        return (patch_col // 2) * AREA + half * 2 * PATCH + (patch_col % 2) * PATCH

    tok_copy.wait()
    tok32[...] = tok_ref[...].astype(jnp.float32)
    for r in range(WIN):
        for p in range(ncols):
            start = base(r // HALF, p) + (r % HALF) * HALF
            x32[start : start + HALF, :] = tok32[r, p * HALF : (p + 1) * HALF, :]

    def block(layer, hooks):
        for w in range(nwin):
            rows = slice(w * AREA, (w + 1) * AREA)
            normed[rows, :] = layer_norm(
                x32[rows, :], gain_ref[layer, 0:1, :], mbias_ref[layer, 0:1, :]
            ).astype(jnp.bfloat16)
        hooks[0]()
        for c in range(3):
            cols = slice(c * channels, (c + 1) * channels)
            qkv_ref[:, cols] = (
                jnp.dot(normed[...], wqkv[layer, :, cols], preferred_element_type=jnp.float32)
                + qkvb_ref[layer : layer + 1, cols]
            ).astype(jnp.bfloat16)
        if layer == 0:
            pos_copy.wait()
        for w in range(nwin):
            hooks[1 + w]()
            rows = slice(w * AREA, (w + 1) * AREA)

            def one_group(g, carry):
                def lanes_of(which):
                    first = pl.multiple_of(which * channels + g * lanes, lanes)
                    return qkv_ref[rows, pl.ds(first, lanes)]

                q, k, v = lanes_of(0), lanes_of(1), lanes_of(2)
                stacked = jnp.concatenate([q * m for m in head_masks], axis=0)
                scores = lax.dot_general(
                    k, stacked, (((1,), (1,)), ((), ())), preferred_element_type=jnp.float32
                )
                scores = scores * (LOG2E / float(np.sqrt(head_dim))) + pos_ref[layer, g]
                if layer == 1:
                    differs = rowdiff[...] * last_row
                    if w == nwin - 1:
                        differs = differs + coldiff[...] * last_col
                    scores = jnp.where(differs > 0.0, -1000000000.0 * LOG2E, scores)
                top = jnp.max(scores, axis=0, keepdims=True)
                weight = jnp.exp2(scores - top)
                total = jnp.sum(weight, axis=0, keepdims=True)
                mixed = lax.dot_general(
                    v, weight.astype(jnp.bfloat16), (((0,), (0,)), ((), ())), preferred_element_type=jnp.float32
                )
                mixed = jnp.where(own_head, mixed * (1.0 / total), 0.0).astype(jnp.bfloat16)
                gathered = lax.dot_general(
                    pick, mixed, (((1,), (1,)), ((), ())), preferred_element_type=jnp.float32
                )
                heads_ref[rows, pl.ds(pl.multiple_of(g * lanes, lanes), lanes)] = gathered.astype(jnp.bfloat16)
                return carry

            lax.fori_loop(0, HEADS // GROUP, one_group, 0)
        hooks[1 + nwin]()
        y32[...] = x32[...] + (
            jnp.dot(heads_ref[...], wproj[layer], preferred_element_type=jnp.float32)
            + mbias_ref[layer, 2:3, :]
        )
        for w in range(nwin):
            rows = slice(w * AREA, (w + 1) * AREA)
            normed[rows, :] = layer_norm(
                y32[rows, :], gain_ref[layer, 1:2, :], mbias_ref[layer, 1:2, :]
            ).astype(jnp.bfloat16)
        hooks[2 + nwin]()
        chunk = 512
        for c in range(whid.shape[2] // chunk):
            cols = slice(c * chunk, (c + 1) * chunk)
            pre = (
                jnp.dot(normed[...], whid[layer, :, cols], preferred_element_type=jnp.float32)
                + hidb_ref[layer : layer + 1, cols]
            )
            hidden_ref[:, cols] = (0.5 * pre * (1.0 + lax.erf(pre * float(np.sqrt(0.5))))).astype(jnp.bfloat16)
        hooks[3 + nwin]()
        final = y32[...] + (
            jnp.dot(hidden_ref[...], wout[layer], preferred_element_type=jnp.float32)
            + mbias_ref[layer, 3:4, :]
        )
        y32[...] = final.astype(jnp.bfloat16).astype(jnp.float32)

    def exchange(k, targets, patches):
        copies = []
        bufs = ((sa, ra), (sb, rb), (sc, rc))
        for which, (source, landing) in enumerate(bufs):
            listed = patches[which]
            for at, (half, p) in enumerate(listed):
                first = base(half, p)
                stage[at * PATCH : (at + 1) * PATCH, :] = y32[first : first + PATCH, :]
            source[k] = stage[0 : len(listed) * PATCH, :].astype(jnp.bfloat16)
            copy = remote(source.at[k], landing.at[k], hsend.at[k, which], hrecv.at[k, which], targets[which])
            copy.start()
            copies.append(copy)
        return copies

    def nothing():
        pass

    def steps(*calls):
        def run():
            for call, t in calls:
                call(t)

        return run

    block(0, [
        steps((forward_x, 0), (forward_x, 1), (forward_y, 0), (ready, 0)),
        steps((forward_y, 1)),
        steps((forward_x, 2)),
        nothing,
        steps((forward_x, 3), (forward_y, 2), (ready, 1)),
        steps((ready, 2),),
        steps((forward_y, 3), (forward_x, 4), (ready, 3)),
    ])
    copies = exchange(0, back, (
        [(0, p) for p in range(1, ncols)], [(1, 0)], [(0, 0)],
    ))
    for p in range(1, ncols):
        first, at = base(1, p), base(0, p - 1)
        x32[at : at + PATCH, :] = y32[first : first + PATCH, :]
    steps((forward_y, 4), (forward_x, 5), (forward_x, 6), (forward_y, 5))()
    for copy in copies:
        copy.wait()
    stage[...] = ra[0].astype(jnp.float32)
    for p in range(ncols - 1):
        at = base(1, p)
        x32[at : at + PATCH, :] = stage[p * PATCH : (p + 1) * PATCH, :]
    at = base(0, ncols - 1)
    x32[at : at + PATCH, :] = rb[0].astype(jnp.float32)
    at = base(1, ncols - 1)
    x32[at : at + PATCH, :] = rc[0].astype(jnp.float32)

    block(1, [
        steps((ready, 4)),
        steps((forward_y, 6)),
        steps((forward_x, 7)),
        nothing,
        steps((forward_y, 7), (ready, 5)),
        steps((ready, 6),),
        steps((ready, 7)),
    ])
    copies = exchange(1, forth, (
        [(1, p) for p in range(ncols - 1)], [(0, ncols - 1)], [(1, ncols - 1)],
    ))

    def put(source, start, half, p):
        for r in range(HALF):
            tok32[half * HALF + r, p * HALF : (p + 1) * HALF, :] = source[
                start + r * HALF : start + (r + 1) * HALF, :
            ]

    for p in range(ncols - 1):
        put(y32, base(0, p), 1, p + 1)
    for copy in copies:
        copy.wait()
    stage[...] = ra[1].astype(jnp.float32)
    for p in range(ncols - 1):
        put(stage, p * PATCH, 0, p + 1)
    stage[0:PATCH, :] = rb[1].astype(jnp.float32)
    stage[PATCH : 2 * PATCH, :] = rc[1].astype(jnp.float32)
    put(stage, 0, 1, 0)
    put(stage, PATCH, 0, 0)
    out_ref[...] = tok32[...].astype(jnp.bfloat16)
    for copy in sends:
        copy.wait_send()


def local(sizes, tokens, qkv_w, proj_w, hid_w, out_w, gain, mbias, qkvb, hidb, position):
    pos = position_tables(position)
    n_col, n_img = sizes[1], sizes[2]
    chips = n_col // 2
    height, width, channels = tokens.shape
    count = height * width
    f32, bf16 = jnp.float32, jnp.bfloat16
    hop = (width // HALF - 1) * PATCH
    dma = pltpu.SemaphoreType.DMA

    def full(w):
        return pltpu.VMEM((w.shape[0], w.shape[1] * n_col, w.shape[2]), bf16)

    any_spec = pl.BlockSpec(memory_space=pl.ANY)
    vmem_spec = pl.BlockSpec(memory_space=pltpu.VMEM)
    return pl.pallas_call(
        functools.partial(kernel, sizes),
        out_shape=jax.ShapeDtypeStruct(tokens.shape, bf16),
        in_specs=[any_spec] * 5 + [vmem_spec] * 4 + [any_spec],
        out_specs=vmem_spec,
        scratch_shapes=[
            full(qkv_w), full(proj_w), full(hid_w), full(out_w),
            pltpu.VMEM(pos.shape, f32),
            pltpu.VMEM(tokens.shape, bf16),
            pltpu.VMEM(tokens.shape, f32),
            pltpu.VMEM((count, channels), f32),
            pltpu.VMEM((count, channels), bf16),
            pltpu.VMEM((count, 3 * channels), bf16),
            pltpu.VMEM((count, channels), bf16),
            pltpu.VMEM((count, hid_w.shape[2]), bf16),
            pltpu.VMEM((count, channels), f32),
            pltpu.VMEM((hop, channels), f32),
            pltpu.VMEM((AREA, GROUP * AREA), f32),
            pltpu.VMEM((AREA, GROUP * AREA), f32),
            pltpu.VMEM((2, hop, channels), bf16),
            pltpu.VMEM((2, PATCH, channels), bf16),
            pltpu.VMEM((2, PATCH, channels), bf16),
            pltpu.VMEM((2, hop, channels), bf16),
            pltpu.VMEM((2, PATCH, channels), bf16),
            pltpu.VMEM((2, PATCH, channels), bf16),
            dma((10,)),
            dma((8,)), dma((8,)),
            dma((8, chips - 1)), dma((8, chips - 1)),
            dma((8, chips - 1)), dma((8, chips - 1)),
            dma((8, chips - 1, 2)), dma((8, chips - 1, 2)),
            dma((2, 3)), dma((2, 3)),
        ],
        compiler_params=pltpu.CompilerParams(
            collective_id=0, has_side_effects=True, vmem_limit_bytes=62 * 1024 * 1024
        ),
        name="swin_pair",
    )(tokens, qkv_w, proj_w, hid_w, out_w, gain, mbias, qkvb, hidb, pos)


def solution(mesh):
    in_specs = (P(("img", "row"), "col", None),) + (P(None, "col", None),) * 4 + (P(),) * 5
    sizes = tuple(mesh.shape[a] for a in ("row", "col", "img"))
    return jax.shard_map(
        functools.partial(local, sizes),
        mesh=mesh,
        in_specs=in_specs,
        out_specs=P(("img", "row"), "col", None),
        check_vma=False,
    )
```

```python
import functools

import jax
import jax.numpy as jnp
import numpy as np
from jax import lax
from jax.experimental import pallas as pl
from jax.experimental.pallas import tpu as pltpu
from jax.sharding import PartitionSpec as P

HEADS = 16
WIN = 12
SHIFT = 6
HALF = WIN // 2
PATCH = HALF * HALF
AREA = WIN * WIN
GROUP = 4
LOG2E = 1.4426950408889634
MESH = pl.DeviceIdType.MESH


def position_rows(table):
    layers, heads, span, _ = table.shape
    groups = heads // GROUP
    flipped = (table * LOG2E)[:, :, :, ::-1].reshape(layers, groups, GROUP, span, span)
    flipped = jnp.pad(flipped.transpose(0, 1, 4, 2, 3), ((0, 0), (0, 0), (0, 1), (0, 0), (0, 1)))
    flat = flipped.reshape(layers * groups * 2 * WIN, GROUP * 2 * WIN)
    return jnp.pad(flat, ((0, 0), (0, 128 - flat.shape[1])))


def layer_norm(values, gain, shift):
    center = values - jnp.mean(values, -1, keepdims=True)
    spread = jnp.mean(center * center, -1, keepdims=True)
    return center * lax.rsqrt(spread + 1e-05) * gain + shift


def kernel(
    sizes,
    tokens_hbm, qkv_hbm, proj_hbm, hid_hbm, outw_hbm,
    gain_ref, mbias_ref, qkvb_ref, hidb_ref, table_ref,
    out_ref,
    wqkv, wproj, whid, wout, pos_ref, tok_ref, tok32, x32, normed, qkv_ref, heads_ref, hidden_ref, y32,
    stage, rowdiff, coldiff, zrows,
    sa, sb, sc, ra, rb, rc,
    local_sem, psend, precv, xsend, xrecv, ysend, yrecv, fsend, frecv, hsend, hrecv,
):
    n_row, n_col, n_img = sizes
    chips = n_col // 2
    row, col, img = lax.axis_index("row"), lax.axis_index("col"), lax.axis_index("img")
    chip, core = col // 2, col % 2
    channels = x32.shape[1]
    nwin = x32.shape[0] // AREA
    ncols = 2 * nwin
    partner = {"col": chip * 2 + (1 - core)}
    ypeer = {"img": (img + 1) % n_img}

    def xpeer(t):
        return {"col": lax.rem(chip + t, chips) * 2 + core}

    up, down = lax.rem(row + n_row - 1, n_row), lax.rem(row + 1, n_row)
    left, right = lax.rem(col + n_col - 1, n_col), lax.rem(col + 1, n_col)
    back = ({"row": up}, {"col": left}, {"row": up, "col": left})
    forth = ({"row": down}, {"col": right}, {"row": down, "col": right})

    barrier = pltpu.get_barrier_semaphore()
    greet = [partner, ypeer, *(xpeer(t) for t in range(1, chips)), *back, *forth]
    for target in greet:
        pl.semaphore_signal(barrier, inc=1, device_id=target, device_id_type=MESH)
    tok_copy = pltpu.make_async_copy(tokens_hbm, tok_ref, local_sem.at[8])
    tok_copy.start()
    pl.semaphore_wait(barrier, len(greet))

    hbm = (qkv_hbm, proj_hbm, hid_hbm, outw_hbm)
    vmem = (wqkv, wproj, whid, wout)
    halves = n_img

    def shard(kind, layer, owner):
        rows = hbm[kind].shape[1]
        return vmem[kind].at[layer, pl.ds(pl.multiple_of(owner * rows, rows), rows), :]

    def part(kind, layer, owner, half):
        rows = hbm[kind].shape[1]
        size = rows // halves
        return vmem[kind].at[layer, pl.ds(pl.multiple_of(owner * rows + half * size, size), size), :]

    def remote(src, dst, send, recv, target):
        return pltpu.make_async_remote_copy(
            src_ref=src, dst_ref=dst, send_sem=send, recv_sem=recv, device_id=target, device_id_type=MESH
        )

    sends = []
    for t in range(8):
        layer, kind = divmod(t, 4)
        rows = hbm[kind].shape[1]
        size = rows // halves
        mine = hbm[kind].at[layer, pl.ds(pl.multiple_of(img * size, size), size), :]
        for d in range(1, chips):
            copy = remote(mine, part(kind, layer, col, img), xsend.at[t, d - 1], xrecv.at[t, d - 1], xpeer(d))
            copy.start()
            sends.append(copy)
        copy = remote(hbm[kind].at[layer], shard(kind, layer, col), psend.at[t], precv.at[t], partner)
        copy.start()
        sends.append(copy)
        pltpu.make_async_copy(hbm[kind].at[layer], shard(kind, layer, col), local_sem.at[t]).start()

    def owner_at(d, lane):
        return lax.rem(chip + chips - d, chips) * 2 + lane

    def forward_x(t):
        layer, kind = divmod(t, 4)
        for d in range(1, chips):
            got = part(kind, layer, owner_at(d, core), img)
            remote(got, got, xsend.at[t, d - 1], xrecv.at[t, d - 1], xpeer(d)).wait_recv()
            for copy in (
                remote(got, got, ysend.at[t, d - 1], yrecv.at[t, d - 1], ypeer),
                remote(got, got, fsend.at[t, d - 1, 0], frecv.at[t, d - 1, 0], partner),
            ):
                copy.start()
                sends.append(copy)

    def forward_y(t):
        layer, kind = divmod(t, 4)
        for d in range(1, chips):
            got = part(kind, layer, owner_at(d, core), 1 - img)
            remote(got, got, ysend.at[t, d - 1], yrecv.at[t, d - 1], ypeer).wait_recv()
            copy = remote(got, got, fsend.at[t, d - 1, 1], frecv.at[t, d - 1, 1], partner)
            copy.start()
            sends.append(copy)

    def ready(t):
        layer, kind = divmod(t, 4)
        pltpu.make_async_copy(hbm[kind].at[layer], shard(kind, layer, col), local_sem.at[t]).wait()
        other = shard(kind, layer, chip * 2 + (1 - core))
        remote(other, other, psend.at[t], precv.at[t], partner).wait_recv()
        for d in range(1, chips):
            for k, half in ((0, img), (1, 1 - img)):
                got = part(kind, layer, owner_at(d, 1 - core), half)
                remote(got, got, fsend.at[t, d - 1, k], frecv.at[t, d - 1, k], partner).wait_recv()

    def iota(shape, dim):
        return lax.broadcasted_iota(jnp.int32, shape, dim)

    wide = GROUP * AREA
    key = iota((AREA, wide), 0)
    query = iota((AREA, wide), 1) % AREA
    rowdiff[...] = ((key // (2 * PATCH)) != (query // (2 * PATCH))).astype(jnp.float32)
    coldiff[...] = (((key // PATCH) % 2) != ((query // PATCH) % 2)).astype(jnp.float32)
    pick = (key == query).astype(jnp.bfloat16)
    head_dim = channels // HEADS
    lanes = GROUP * head_dim
    own_head = iota((lanes, wide), 0) // head_dim == iota((lanes, wide), 1) // AREA
    head_masks = [(iota((AREA, lanes), 1) // head_dim == h).astype(jnp.bfloat16) for h in range(GROUP)]
    last_row = (row == n_row - 1).astype(jnp.float32)
    last_col = (col == n_col - 1).astype(jnp.float32)

    def base(half, patch_col):
        return (patch_col // 2) * AREA + half * 2 * PATCH + (patch_col % 2) * PATCH

    tok_copy.wait()
    tok32[...] = tok_ref[...].astype(jnp.float32)
    for r in range(WIN):
        for p in range(ncols):
            start = base(r // HALF, p) + (r % HALF) * HALF
            x32[start : start + HALF, :] = tok32[r, p * HALF : (p + 1) * HALF, :]

    span = 2 * WIN
    high = table_ref[...].astype(jnp.bfloat16)
    rest = table_ref[...] - high.astype(jnp.float32)
    middle = rest.astype(jnp.bfloat16)
    low = (rest - middle.astype(jnp.float32)).astype(jnp.bfloat16)
    thirds = jnp.concatenate([high, middle, low], axis=0)
    count = table_ref.shape[0]

    def positions(rb):
        slot = iota((table_ref.shape[1], wide), 0)
        lane = iota((table_ref.shape[1], wide), 1)
        at = lane % AREA
        ra = (at // (2 * PATCH)) * HALF + (at % PATCH) // HALF
        onehot = (slot == (lane // AREA) * span + ra - rb + WIN - 1).astype(jnp.bfloat16)
        found = jnp.dot(thirds, onehot, preferred_element_type=jnp.float32)
        found = found[:count] + found[count : 2 * count] + found[2 * count :]
        zrows[...] = found.reshape(zrows.shape)
        inner = iota((1, wide), 1) % AREA
        ca = ((inner // PATCH) % 2) * HALF + inner % HALF

        def one(n, carry):
            rows = jnp.zeros((WIN, wide), jnp.float32)
            for v in range(WIN):
                rows = jnp.where(ca == v, zrows[n, WIN - 1 - v : 2 * WIN - 1 - v, :], rows)
            groups = HEADS // GROUP
            for pc in range(2):
                first = (rb // HALF) * 2 * PATCH + pc * PATCH + (rb % HALF) * HALF
                pos_ref[n // groups, n % groups, first : first + HALF, :] = rows[pc * HALF : (pc + 1) * HALF]
            return carry

        lax.fori_loop(0, zrows.shape[0], one, 0)

    def position_range(rows):
        for rb in rows:
            positions(rb)

    def block(layer, hooks):
        for w in range(nwin):
            rows = slice(w * AREA, (w + 1) * AREA)
            normed[rows, :] = layer_norm(
                x32[rows, :], gain_ref[layer, 0:1, :], mbias_ref[layer, 0:1, :]
            ).astype(jnp.bfloat16)
        hooks[0]()
        for c in range(3):
            cols = slice(c * channels, (c + 1) * channels)
            qkv_ref[:, cols] = (
                jnp.dot(normed[...], wqkv[layer, :, cols], preferred_element_type=jnp.float32)
                + qkvb_ref[layer : layer + 1, cols]
            ).astype(jnp.bfloat16)
        for w in range(nwin):
            hooks[1 + w]()
            rows = slice(w * AREA, (w + 1) * AREA)

            def one_group(g, carry):
                def lanes_of(which):
                    first = pl.multiple_of(which * channels + g * lanes, lanes)
                    return qkv_ref[rows, pl.ds(first, lanes)]

                q, k, v = lanes_of(0), lanes_of(1), lanes_of(2)
                stacked = jnp.concatenate([q * m for m in head_masks], axis=0)
                scores = lax.dot_general(
                    k, stacked, (((1,), (1,)), ((), ())), preferred_element_type=jnp.float32
                )
                scores = scores * (LOG2E / float(np.sqrt(head_dim))) + pos_ref[layer, g]
                if layer == 1:
                    differs = rowdiff[...] * last_row
                    if w == nwin - 1:
                        differs = differs + coldiff[...] * last_col
                    scores = jnp.where(differs > 0.0, -1000000000.0 * LOG2E, scores)
                top = jnp.max(scores, axis=0, keepdims=True)
                weight = jnp.exp2(scores - top)
                total = jnp.sum(weight, axis=0, keepdims=True)
                mixed = lax.dot_general(
                    v, weight.astype(jnp.bfloat16), (((0,), (0,)), ((), ())), preferred_element_type=jnp.float32
                )
                mixed = jnp.where(own_head, mixed * (1.0 / total), 0.0).astype(jnp.bfloat16)
                gathered = lax.dot_general(
                    pick, mixed, (((1,), (1,)), ((), ())), preferred_element_type=jnp.float32
                )
                heads_ref[rows, pl.ds(pl.multiple_of(g * lanes, lanes), lanes)] = gathered.astype(jnp.bfloat16)
                return carry

            lax.fori_loop(0, HEADS // GROUP, one_group, 0)
        hooks[1 + nwin]()
        y32[...] = x32[...] + (
            jnp.dot(heads_ref[...], wproj[layer], preferred_element_type=jnp.float32)
            + mbias_ref[layer, 2:3, :]
        )
        for w in range(nwin):
            rows = slice(w * AREA, (w + 1) * AREA)
            normed[rows, :] = layer_norm(
                y32[rows, :], gain_ref[layer, 1:2, :], mbias_ref[layer, 1:2, :]
            ).astype(jnp.bfloat16)
        hooks[2 + nwin]()
        chunk = 512
        for c in range(whid.shape[2] // chunk):
            cols = slice(c * chunk, (c + 1) * chunk)
            pre = (
                jnp.dot(normed[...], whid[layer, :, cols], preferred_element_type=jnp.float32)
                + hidb_ref[layer : layer + 1, cols]
            )
            hidden_ref[:, cols] = (0.5 * pre * (1.0 + lax.erf(pre * float(np.sqrt(0.5))))).astype(jnp.bfloat16)
        hooks[3 + nwin]()
        final = y32[...] + (
            jnp.dot(hidden_ref[...], wout[layer], preferred_element_type=jnp.float32)
            + mbias_ref[layer, 3:4, :]
        )
        y32[...] = final.astype(jnp.bfloat16).astype(jnp.float32)

    def exchange(k, targets, patches):
        copies = []
        bufs = ((sa, ra), (sb, rb), (sc, rc))
        for which, (source, landing) in enumerate(bufs):
            listed = patches[which]
            for at, (half, p) in enumerate(listed):
                first = base(half, p)
                stage[at * PATCH : (at + 1) * PATCH, :] = y32[first : first + PATCH, :]
            source[k] = stage[0 : len(listed) * PATCH, :].astype(jnp.bfloat16)
            copy = remote(source.at[k], landing.at[k], hsend.at[k, which], hrecv.at[k, which], targets[which])
            copy.start()
            copies.append(copy)
        return copies

    def nothing():
        pass

    def steps(*calls):
        def run():
            for call, t in calls:
                call(t)

        return run

    block(0, [
        steps(
            (position_range, range(0, 5)), (forward_x, 0), (position_range, range(5, 8)), (forward_x, 1),
            (position_range, range(8, WIN)), (forward_y, 0), (ready, 0),
        ),
        steps((forward_y, 1)),
        steps((forward_x, 2)),
        nothing,
        steps((forward_x, 3), (forward_y, 2), (ready, 1)),
        steps((ready, 2),),
        steps((forward_y, 3), (forward_x, 4), (ready, 3)),
    ])
    copies = exchange(0, back, (
        [(0, p) for p in range(1, ncols)], [(1, 0)], [(0, 0)],
    ))
    for p in range(1, ncols):
        first, at = base(1, p), base(0, p - 1)
        x32[at : at + PATCH, :] = y32[first : first + PATCH, :]
    steps((forward_y, 4), (forward_x, 5), (forward_x, 6), (forward_y, 5))()
    for copy in copies:
        copy.wait()
    stage[...] = ra[0].astype(jnp.float32)
    for p in range(ncols - 1):
        at = base(1, p)
        x32[at : at + PATCH, :] = stage[p * PATCH : (p + 1) * PATCH, :]
    at = base(0, ncols - 1)
    x32[at : at + PATCH, :] = rb[0].astype(jnp.float32)
    at = base(1, ncols - 1)
    x32[at : at + PATCH, :] = rc[0].astype(jnp.float32)

    block(1, [
        steps((ready, 4)),
        steps((forward_y, 6)),
        steps((forward_x, 7)),
        nothing,
        steps((forward_y, 7), (ready, 5)),
        steps((ready, 6),),
        steps((ready, 7)),
    ])
    copies = exchange(1, forth, (
        [(1, p) for p in range(ncols - 1)], [(0, ncols - 1)], [(1, ncols - 1)],
    ))

    def put(source, start, half, p):
        for r in range(HALF):
            tok32[half * HALF + r, p * HALF : (p + 1) * HALF, :] = source[
                start + r * HALF : start + (r + 1) * HALF, :
            ]

    for p in range(ncols - 1):
        put(y32, base(0, p), 1, p + 1)
    for copy in copies:
        copy.wait()
    stage[...] = ra[1].astype(jnp.float32)
    for p in range(ncols - 1):
        put(stage, p * PATCH, 0, p + 1)
    stage[0:PATCH, :] = rb[1].astype(jnp.float32)
    stage[PATCH : 2 * PATCH, :] = rc[1].astype(jnp.float32)
    put(stage, 0, 1, 0)
    put(stage, PATCH, 0, 0)
    out_ref[...] = tok32[...].astype(jnp.bfloat16)
    for copy in sends:
        copy.wait_send()


def local(sizes, tokens, qkv_w, proj_w, hid_w, out_w, gain, mbias, qkvb, hidb, position):
    table = position_rows(position)
    n_col, n_img = sizes[1], sizes[2]
    chips = n_col // 2
    height, width, channels = tokens.shape
    count = height * width
    f32, bf16 = jnp.float32, jnp.bfloat16
    hop = (width // HALF - 1) * PATCH
    dma = pltpu.SemaphoreType.DMA

    def full(w):
        return pltpu.VMEM((w.shape[0], w.shape[1] * n_col, w.shape[2]), bf16)

    any_spec = pl.BlockSpec(memory_space=pl.ANY)
    vmem_spec = pl.BlockSpec(memory_space=pltpu.VMEM)
    return pl.pallas_call(
        functools.partial(kernel, sizes),
        out_shape=jax.ShapeDtypeStruct(tokens.shape, bf16),
        in_specs=[any_spec] * 5 + [vmem_spec] * 5,
        out_specs=vmem_spec,
        scratch_shapes=[
            full(qkv_w), full(proj_w), full(hid_w), full(out_w),
            pltpu.VMEM((2, HEADS // GROUP, AREA, GROUP * AREA), f32),
            pltpu.VMEM(tokens.shape, bf16),
            pltpu.VMEM(tokens.shape, f32),
            pltpu.VMEM((count, channels), f32),
            pltpu.VMEM((count, channels), bf16),
            pltpu.VMEM((count, 3 * channels), bf16),
            pltpu.VMEM((count, channels), bf16),
            pltpu.VMEM((count, hid_w.shape[2]), bf16),
            pltpu.VMEM((count, channels), f32),
            pltpu.VMEM((hop, channels), f32),
            pltpu.VMEM((AREA, GROUP * AREA), f32),
            pltpu.VMEM((AREA, GROUP * AREA), f32),
            pltpu.VMEM((2 * HEADS // GROUP, 2 * WIN, GROUP * AREA), f32),
            pltpu.VMEM((2, hop, channels), bf16),
            pltpu.VMEM((2, PATCH, channels), bf16),
            pltpu.VMEM((2, PATCH, channels), bf16),
            pltpu.VMEM((2, hop, channels), bf16),
            pltpu.VMEM((2, PATCH, channels), bf16),
            pltpu.VMEM((2, PATCH, channels), bf16),
            dma((10,)),
            dma((8,)), dma((8,)),
            dma((8, chips - 1)), dma((8, chips - 1)),
            dma((8, chips - 1)), dma((8, chips - 1)),
            dma((8, chips - 1, 2)), dma((8, chips - 1, 2)),
            dma((2, 3)), dma((2, 3)),
        ],
        compiler_params=pltpu.CompilerParams(
            collective_id=0, has_side_effects=True, vmem_limit_bytes=62 * 1024 * 1024
        ),
        name="swin_pair",
    )(tokens, qkv_w, proj_w, hid_w, out_w, gain, mbias, qkvb, hidb, table)


def solution(mesh):
    in_specs = (P(("img", "row"), "col", None),) + (P(None, "col", None),) * 4 + (P(),) * 5
    sizes = tuple(mesh.shape[a] for a in ("row", "col", "img"))
    return jax.shard_map(
        functools.partial(local, sizes),
        mesh=mesh,
        in_specs=in_specs,
        out_specs=P(("img", "row"), "col", None),
        check_vma=False,
    )
```

```python
import functools

import jax
import jax.numpy as jnp
import numpy as np
from jax import lax
from jax.experimental import pallas as pl
from jax.experimental.pallas import tpu as pltpu
from jax.sharding import PartitionSpec as P

HEADS = 16
WIN = 12
SHIFT = 6
HALF = WIN // 2
PATCH = HALF * HALF
AREA = WIN * WIN
GROUP = 4
LOG2E = 1.4426950408889634
MESH = pl.DeviceIdType.MESH


def position_rows(table):
    layers, heads, span, _ = table.shape
    groups = heads // GROUP
    flipped = (table * LOG2E)[:, :, :, ::-1].reshape(layers, groups, GROUP, span, span)
    flipped = jnp.pad(flipped.transpose(0, 1, 4, 2, 3), ((0, 0), (0, 0), (0, 1), (0, 0), (0, 1)))
    flat = flipped.reshape(layers * groups * 2 * WIN, GROUP * 2 * WIN)
    return jnp.pad(flat, ((0, 0), (0, 128 - flat.shape[1])))


def layer_norm(values, gain, shift):
    center = values - jnp.mean(values, -1, keepdims=True)
    spread = jnp.mean(center * center, -1, keepdims=True)
    return center * lax.rsqrt(spread + 1e-05) * gain + shift


def kernel(
    sizes,
    tokens_hbm, qkv_hbm, proj_hbm, hid_hbm, outw_hbm,
    gain_ref, mbias_ref, qkvb_ref, hidb_ref, table_ref,
    out_ref,
    wqkv, wproj, whid, wout, pos_ref, tok_ref, tok32, x32, normed, qkv_ref, heads_ref, hidden_ref, y32,
    stage, rowdiff, coldiff, zrows,
    sa, sb, sc, ra, rb, rc,
    local_sem, psend, precv, xsend, xrecv, ysend, yrecv, fsend, frecv, hsend, hrecv,
):
    n_row, n_col, n_img = sizes
    chips = n_col // 2
    row, col, img = lax.axis_index("row"), lax.axis_index("col"), lax.axis_index("img")
    chip, core = col // 2, col % 2
    channels = x32.shape[1]
    nwin = x32.shape[0] // AREA
    ncols = 2 * nwin
    partner = {"col": chip * 2 + (1 - core)}
    ypeer = {"img": (img + 1) % n_img}

    def xpeer(t):
        return {"col": lax.rem(chip + t, chips) * 2 + core}

    up, down = lax.rem(row + n_row - 1, n_row), lax.rem(row + 1, n_row)
    left, right = lax.rem(col + n_col - 1, n_col), lax.rem(col + 1, n_col)
    back = ({"row": up}, {"col": left}, {"row": up, "col": left})
    forth = ({"row": down}, {"col": right}, {"row": down, "col": right})

    barrier = pltpu.get_barrier_semaphore()
    greet = [partner, ypeer, *(xpeer(t) for t in range(1, chips)), *back, *forth]
    for target in greet:
        pl.semaphore_signal(barrier, inc=1, device_id=target, device_id_type=MESH)
    tok_copy = pltpu.make_async_copy(tokens_hbm, tok_ref, local_sem.at[8])
    tok_copy.start()
    pl.semaphore_wait(barrier, len(greet))

    hbm = (qkv_hbm, proj_hbm, hid_hbm, outw_hbm)
    vmem = (wqkv, wproj, whid, wout)
    halves = n_img

    def shard(kind, layer, owner):
        rows = hbm[kind].shape[1]
        return vmem[kind].at[layer, pl.ds(pl.multiple_of(owner * rows, rows), rows), :]

    def part(kind, layer, owner, half):
        rows = hbm[kind].shape[1]
        size = rows // halves
        return vmem[kind].at[layer, pl.ds(pl.multiple_of(owner * rows + half * size, size), size), :]

    def remote(src, dst, send, recv, target):
        return pltpu.make_async_remote_copy(
            src_ref=src, dst_ref=dst, send_sem=send, recv_sem=recv, device_id=target, device_id_type=MESH
        )

    sends = []
    for t in range(8):
        layer, kind = divmod(t, 4)
        rows = hbm[kind].shape[1]
        size = rows // halves
        mine = hbm[kind].at[layer, pl.ds(pl.multiple_of(img * size, size), size), :]
        for d in range(1, chips):
            copy = remote(mine, part(kind, layer, col, img), xsend.at[t, d - 1], xrecv.at[t, d - 1], xpeer(d))
            copy.start()
            sends.append(copy)
        copy = remote(hbm[kind].at[layer], shard(kind, layer, col), psend.at[t], precv.at[t], partner)
        copy.start()
        sends.append(copy)
        pltpu.make_async_copy(hbm[kind].at[layer], shard(kind, layer, col), local_sem.at[t]).start()

    def owner_at(d, lane):
        return lax.rem(chip + chips - d, chips) * 2 + lane

    def forward_x(t):
        layer, kind = divmod(t, 4)
        for d in range(1, chips):
            got = part(kind, layer, owner_at(d, core), img)
            remote(got, got, xsend.at[t, d - 1], xrecv.at[t, d - 1], xpeer(d)).wait_recv()
            for copy in (
                remote(got, got, ysend.at[t, d - 1], yrecv.at[t, d - 1], ypeer),
                remote(got, got, fsend.at[t, d - 1, 0], frecv.at[t, d - 1, 0], partner),
            ):
                copy.start()
                sends.append(copy)

    def forward_y(t):
        layer, kind = divmod(t, 4)
        for d in range(1, chips):
            got = part(kind, layer, owner_at(d, core), 1 - img)
            remote(got, got, ysend.at[t, d - 1], yrecv.at[t, d - 1], ypeer).wait_recv()
            copy = remote(got, got, fsend.at[t, d - 1, 1], frecv.at[t, d - 1, 1], partner)
            copy.start()
            sends.append(copy)

    def ready(t):
        layer, kind = divmod(t, 4)
        pltpu.make_async_copy(hbm[kind].at[layer], shard(kind, layer, col), local_sem.at[t]).wait()
        other = shard(kind, layer, chip * 2 + (1 - core))
        remote(other, other, psend.at[t], precv.at[t], partner).wait_recv()
        for d in range(1, chips):
            for k, half in ((0, img), (1, 1 - img)):
                got = part(kind, layer, owner_at(d, 1 - core), half)
                remote(got, got, fsend.at[t, d - 1, k], frecv.at[t, d - 1, k], partner).wait_recv()

    def iota(shape, dim):
        return lax.broadcasted_iota(jnp.int32, shape, dim)

    wide = GROUP * AREA
    key = iota((AREA, wide), 0)
    query = iota((AREA, wide), 1) % AREA
    rowdiff[...] = ((key // (2 * PATCH)) != (query // (2 * PATCH))).astype(jnp.float32)
    coldiff[...] = (((key // PATCH) % 2) != ((query // PATCH) % 2)).astype(jnp.float32)
    pick = (key == query).astype(jnp.bfloat16)
    head_dim = channels // HEADS
    lanes = GROUP * head_dim
    own_head = iota((lanes, wide), 0) // head_dim == iota((lanes, wide), 1) // AREA
    head_masks = [(iota((AREA, lanes), 1) // head_dim == h).astype(jnp.bfloat16) for h in range(GROUP)]
    last_row = (row == n_row - 1).astype(jnp.float32)
    last_col = (col == n_col - 1).astype(jnp.float32)

    def base(half, patch_col):
        return (patch_col // 2) * AREA + half * 2 * PATCH + (patch_col % 2) * PATCH

    tok_copy.wait()
    tok32[...] = tok_ref[...].astype(jnp.float32)
    for r in range(WIN):
        for p in range(ncols):
            start = base(r // HALF, p) + (r % HALF) * HALF
            x32[start : start + HALF, :] = tok32[r, p * HALF : (p + 1) * HALF, :]

    span = 2 * WIN
    high = table_ref[...].astype(jnp.bfloat16)
    rest = table_ref[...] - high.astype(jnp.float32)
    middle = rest.astype(jnp.bfloat16)
    low = (rest - middle.astype(jnp.float32)).astype(jnp.bfloat16)
    thirds = jnp.concatenate([high, middle, low], axis=0)
    count = table_ref.shape[0]

    def positions(rb):
        slot = iota((table_ref.shape[1], wide), 0)
        lane = iota((table_ref.shape[1], wide), 1)
        at = lane % AREA
        ra = (at // (2 * PATCH)) * HALF + (at % PATCH) // HALF
        onehot = (slot == (lane // AREA) * span + ra - rb + WIN - 1).astype(jnp.bfloat16)
        found = jnp.dot(thirds, onehot, preferred_element_type=jnp.float32)
        found = found[:count] + found[count : 2 * count] + found[2 * count :]
        zrows[...] = found.reshape(zrows.shape)
        inner = iota((1, wide), 1) % AREA
        ca = ((inner // PATCH) % 2) * HALF + inner % HALF

        def one(n, carry):
            rows = jnp.zeros((WIN, wide), jnp.float32)
            for v in range(WIN):
                rows = jnp.where(ca == v, zrows[n, WIN - 1 - v : 2 * WIN - 1 - v, :], rows)
            groups = HEADS // GROUP
            for pc in range(2):
                first = (rb // HALF) * 2 * PATCH + pc * PATCH + (rb % HALF) * HALF
                pos_ref[n // groups, n % groups, first : first + HALF, :] = rows[pc * HALF : (pc + 1) * HALF]
            return carry

        lax.fori_loop(0, zrows.shape[0], one, 0)

    def position_range(rows):
        for rb in rows:
            positions(rb)

    def block(layer, hooks):
        for w in range(nwin):
            rows = slice(w * AREA, (w + 1) * AREA)
            normed[rows, :] = layer_norm(
                x32[rows, :], gain_ref[layer, 0:1, :], mbias_ref[layer, 0:1, :]
            ).astype(jnp.bfloat16)
        hooks[0]()
        for c in range(3):
            cols = slice(c * channels, (c + 1) * channels)
            qkv_ref[:, cols] = (
                jnp.dot(normed[...], wqkv[layer, :, cols], preferred_element_type=jnp.float32)
                + qkvb_ref[layer : layer + 1, cols]
            ).astype(jnp.bfloat16)
        for w in range(nwin):
            hooks[1 + w]()
            rows = slice(w * AREA, (w + 1) * AREA)

            def one_group(g, carry):
                def lanes_of(which):
                    first = pl.multiple_of(which * channels + g * lanes, lanes)
                    return qkv_ref[rows, pl.ds(first, lanes)]

                q, k, v = lanes_of(0), lanes_of(1), lanes_of(2)
                stacked = jnp.concatenate([q * m for m in head_masks], axis=0)
                scores = lax.dot_general(
                    k, stacked, (((1,), (1,)), ((), ())), preferred_element_type=jnp.float32
                )
                scores = scores * (LOG2E / float(np.sqrt(head_dim))) + pos_ref[layer, g]
                if layer == 1:
                    differs = rowdiff[...] * last_row
                    if w == nwin - 1:
                        differs = differs + coldiff[...] * last_col
                    scores = jnp.where(differs > 0.0, -1000000000.0 * LOG2E, scores)
                top = jnp.max(scores, axis=0, keepdims=True)
                weight = jnp.exp2(scores - top)
                total = jnp.sum(weight, axis=0, keepdims=True)
                mixed = lax.dot_general(
                    v, weight.astype(jnp.bfloat16), (((0,), (0,)), ((), ())), preferred_element_type=jnp.float32
                )
                mixed = jnp.where(own_head, mixed * (1.0 / total), 0.0).astype(jnp.bfloat16)
                gathered = lax.dot_general(
                    pick, mixed, (((1,), (1,)), ((), ())), preferred_element_type=jnp.float32
                )
                heads_ref[rows, pl.ds(pl.multiple_of(g * lanes, lanes), lanes)] = gathered.astype(jnp.bfloat16)
                return carry

            lax.fori_loop(0, HEADS // GROUP, one_group, 0, unroll=4)
        hooks[1 + nwin]()
        y32[...] = x32[...] + (
            jnp.dot(heads_ref[...], wproj[layer], preferred_element_type=jnp.float32)
            + mbias_ref[layer, 2:3, :]
        )
        for w in range(nwin):
            rows = slice(w * AREA, (w + 1) * AREA)
            normed[rows, :] = layer_norm(
                y32[rows, :], gain_ref[layer, 1:2, :], mbias_ref[layer, 1:2, :]
            ).astype(jnp.bfloat16)
        hooks[2 + nwin]()
        chunk = 512
        for c in range(whid.shape[2] // chunk):
            cols = slice(c * chunk, (c + 1) * chunk)
            pre = (
                jnp.dot(normed[...], whid[layer, :, cols], preferred_element_type=jnp.float32)
                + hidb_ref[layer : layer + 1, cols]
            )
            hidden_ref[:, cols] = (0.5 * pre * (1.0 + lax.erf(pre * float(np.sqrt(0.5))))).astype(jnp.bfloat16)
        hooks[3 + nwin]()
        final = y32[...] + (
            jnp.dot(hidden_ref[...], wout[layer], preferred_element_type=jnp.float32)
            + mbias_ref[layer, 3:4, :]
        )
        y32[...] = final.astype(jnp.bfloat16).astype(jnp.float32)

    def exchange(k, targets, patches):
        copies = []
        bufs = ((sa, ra), (sb, rb), (sc, rc))
        for which, (source, landing) in enumerate(bufs):
            listed = patches[which]
            for at, (half, p) in enumerate(listed):
                first = base(half, p)
                stage[at * PATCH : (at + 1) * PATCH, :] = y32[first : first + PATCH, :]
            source[k] = stage[0 : len(listed) * PATCH, :].astype(jnp.bfloat16)
            copy = remote(source.at[k], landing.at[k], hsend.at[k, which], hrecv.at[k, which], targets[which])
            copy.start()
            copies.append(copy)
        return copies

    def nothing():
        pass

    def steps(*calls):
        def run():
            for call, t in calls:
                call(t)

        return run

    block(0, [
        steps(
            (position_range, range(0, 5)), (forward_x, 0), (position_range, range(5, 8)), (forward_x, 1),
            (position_range, range(8, WIN)), (forward_y, 0), (forward_x, 2), (ready, 0),
        ),
        steps((forward_y, 1)),
        nothing,
        steps((forward_x, 3), (forward_y, 2)),
        steps((ready, 1)),
        steps((forward_x, 4), (ready, 2)),
        steps((forward_y, 3), (forward_x, 5), (ready, 3)),
    ])
    copies = exchange(0, back, (
        [(0, p) for p in range(1, ncols)], [(1, 0)], [(0, 0)],
    ))
    for p in range(1, ncols):
        first, at = base(1, p), base(0, p - 1)
        x32[at : at + PATCH, :] = y32[first : first + PATCH, :]
    steps((forward_y, 4), (forward_x, 6), (forward_y, 5))()
    for copy in copies:
        copy.wait()
    stage[...] = ra[0].astype(jnp.float32)
    for p in range(ncols - 1):
        at = base(1, p)
        x32[at : at + PATCH, :] = stage[p * PATCH : (p + 1) * PATCH, :]
    at = base(0, ncols - 1)
    x32[at : at + PATCH, :] = rb[0].astype(jnp.float32)
    at = base(1, ncols - 1)
    x32[at : at + PATCH, :] = rc[0].astype(jnp.float32)

    block(1, [
        steps((ready, 4), (forward_x, 7)),
        steps((forward_y, 6)),
        nothing,
        steps((forward_y, 7)),
        steps((ready, 5)),
        steps((ready, 6)),
        steps((ready, 7)),
    ])
    copies = exchange(1, forth, (
        [(1, p) for p in range(ncols - 1)], [(0, ncols - 1)], [(1, ncols - 1)],
    ))

    def put(source, start, half, p):
        for r in range(HALF):
            tok32[half * HALF + r, p * HALF : (p + 1) * HALF, :] = source[
                start + r * HALF : start + (r + 1) * HALF, :
            ]

    for p in range(ncols - 1):
        put(y32, base(0, p), 1, p + 1)
    for copy in copies:
        copy.wait()
    stage[...] = ra[1].astype(jnp.float32)
    for p in range(ncols - 1):
        put(stage, p * PATCH, 0, p + 1)
    stage[0:PATCH, :] = rb[1].astype(jnp.float32)
    stage[PATCH : 2 * PATCH, :] = rc[1].astype(jnp.float32)
    put(stage, 0, 1, 0)
    put(stage, PATCH, 0, 0)
    out_ref[...] = tok32[...].astype(jnp.bfloat16)
    for copy in sends:
        copy.wait_send()


def local(sizes, tokens, qkv_w, proj_w, hid_w, out_w, gain, mbias, qkvb, hidb, position):
    table = position_rows(position)
    n_col, n_img = sizes[1], sizes[2]
    chips = n_col // 2
    height, width, channels = tokens.shape
    count = height * width
    f32, bf16 = jnp.float32, jnp.bfloat16
    hop = (width // HALF - 1) * PATCH
    dma = pltpu.SemaphoreType.DMA

    def full(w):
        return pltpu.VMEM((w.shape[0], w.shape[1] * n_col, w.shape[2]), bf16)

    any_spec = pl.BlockSpec(memory_space=pl.ANY)
    vmem_spec = pl.BlockSpec(memory_space=pltpu.VMEM)
    return pl.pallas_call(
        functools.partial(kernel, sizes),
        out_shape=jax.ShapeDtypeStruct(tokens.shape, bf16),
        in_specs=[any_spec] * 5 + [vmem_spec] * 5,
        out_specs=vmem_spec,
        scratch_shapes=[
            full(qkv_w), full(proj_w), full(hid_w), full(out_w),
            pltpu.VMEM((2, HEADS // GROUP, AREA, GROUP * AREA), f32),
            pltpu.VMEM(tokens.shape, bf16),
            pltpu.VMEM(tokens.shape, f32),
            pltpu.VMEM((count, channels), f32),
            pltpu.VMEM((count, channels), bf16),
            pltpu.VMEM((count, 3 * channels), bf16),
            pltpu.VMEM((count, channels), bf16),
            pltpu.VMEM((count, hid_w.shape[2]), bf16),
            pltpu.VMEM((count, channels), f32),
            pltpu.VMEM((hop, channels), f32),
            pltpu.VMEM((AREA, GROUP * AREA), f32),
            pltpu.VMEM((AREA, GROUP * AREA), f32),
            pltpu.VMEM((2 * HEADS // GROUP, 2 * WIN, GROUP * AREA), f32),
            pltpu.VMEM((2, hop, channels), bf16),
            pltpu.VMEM((2, PATCH, channels), bf16),
            pltpu.VMEM((2, PATCH, channels), bf16),
            pltpu.VMEM((2, hop, channels), bf16),
            pltpu.VMEM((2, PATCH, channels), bf16),
            pltpu.VMEM((2, PATCH, channels), bf16),
            dma((10,)),
            dma((8,)), dma((8,)),
            dma((8, chips - 1)), dma((8, chips - 1)),
            dma((8, chips - 1)), dma((8, chips - 1)),
            dma((8, chips - 1, 2)), dma((8, chips - 1, 2)),
            dma((2, 3)), dma((2, 3)),
        ],
        compiler_params=pltpu.CompilerParams(
            collective_id=0, has_side_effects=True, vmem_limit_bytes=62 * 1024 * 1024
        ),
        name="swin_pair",
    )(tokens, qkv_w, proj_w, hid_w, out_w, gain, mbias, qkvb, hidb, table)


def solution(mesh):
    in_specs = (P(("img", "row"), "col", None),) + (P(None, "col", None),) * 4 + (P(),) * 5
    sizes = tuple(mesh.shape[a] for a in ("row", "col", "img"))
    return jax.shard_map(
        functools.partial(local, sizes),
        mesh=mesh,
        in_specs=in_specs,
        out_specs=P(("img", "row"), "col", None),
        check_vma=False,
    )
```

```python
import functools

import jax
import jax.numpy as jnp
import numpy as np
from jax import lax
from jax.experimental import pallas as pl
from jax.experimental.pallas import tpu as pltpu
from jax.sharding import PartitionSpec as P

HEADS = 16
WIN = 12
SHIFT = 6
HALF = WIN // 2
PATCH = HALF * HALF
AREA = WIN * WIN
GROUP = 4
LOG2E = 1.4426950408889634
MESH = pl.DeviceIdType.MESH


def position_rows(table):
    layers, heads, span, _ = table.shape
    groups = heads // GROUP
    flipped = (table * LOG2E)[:, :, :, ::-1].reshape(layers, groups, GROUP, span, span)
    flipped = jnp.pad(flipped.transpose(0, 1, 4, 2, 3), ((0, 0), (0, 0), (0, 1), (0, 0), (0, 1)))
    flat = flipped.reshape(layers * groups * 2 * WIN, GROUP * 2 * WIN)
    return jnp.pad(flat, ((0, 0), (0, 128 - flat.shape[1])))


def layer_norm(values, gain, shift):
    center = values - jnp.mean(values, -1, keepdims=True)
    spread = jnp.mean(center * center, -1, keepdims=True)
    return center * lax.rsqrt(spread + 1e-05) * gain + shift


def kernel(
    sizes,
    tokens_hbm, qkv_hbm, proj_hbm, hid_hbm, outw_hbm,
    gain_ref, mbias_ref, qkvb_ref, hidb_ref, table_ref,
    out_ref,
    wqkv, wproj, whid, wout, pos_ref, tok_ref, tok32, x32, normed, qkv_ref, heads_ref, hidden_ref, y32, m32,
    stage, rowdiff, coldiff, zrows,
    sa, sb, sc, ra, rb, rc,
    local_sem, psend, precv, xsend, xrecv, ysend, yrecv, fsend, frecv, hsend, hrecv,
):
    n_row, n_col, n_img = sizes
    chips = n_col // 2
    row, col, img = lax.axis_index("row"), lax.axis_index("col"), lax.axis_index("img")
    chip, core = col // 2, col % 2
    channels = x32.shape[1]
    nwin = x32.shape[0] // AREA
    ncols = 2 * nwin
    partner = {"col": chip * 2 + (1 - core)}
    ypeer = {"img": (img + 1) % n_img}

    def xpeer(t):
        return {"col": lax.rem(chip + t, chips) * 2 + core}

    up, down = lax.rem(row + n_row - 1, n_row), lax.rem(row + 1, n_row)
    left, right = lax.rem(col + n_col - 1, n_col), lax.rem(col + 1, n_col)
    back = ({"row": up}, {"col": left}, {"row": up, "col": left})
    forth = ({"row": down}, {"col": right}, {"row": down, "col": right})

    barrier = pltpu.get_barrier_semaphore()
    greet = [partner, ypeer, *(xpeer(t) for t in range(1, chips)), *back, *forth]
    for target in greet:
        pl.semaphore_signal(barrier, inc=1, device_id=target, device_id_type=MESH)
    tok_copy = pltpu.make_async_copy(tokens_hbm, tok_ref, local_sem.at[8])
    tok_copy.start()
    pl.semaphore_wait(barrier, len(greet))

    hbm = (qkv_hbm, proj_hbm, hid_hbm, outw_hbm)
    vmem = (wqkv, wproj, whid, wout)
    halves = n_img

    def shard(kind, layer, owner):
        rows = hbm[kind].shape[1]
        return vmem[kind].at[layer, pl.ds(pl.multiple_of(owner * rows, rows), rows), :]

    def part(kind, layer, owner, half):
        rows = hbm[kind].shape[1]
        size = rows // halves
        return vmem[kind].at[layer, pl.ds(pl.multiple_of(owner * rows + half * size, size), size), :]

    def remote(src, dst, send, recv, target):
        return pltpu.make_async_remote_copy(
            src_ref=src, dst_ref=dst, send_sem=send, recv_sem=recv, device_id=target, device_id_type=MESH
        )

    sends = []
    for t in range(8):
        layer, kind = divmod(t, 4)
        rows = hbm[kind].shape[1]
        size = rows // halves
        mine = hbm[kind].at[layer, pl.ds(pl.multiple_of(img * size, size), size), :]
        for d in range(1, chips):
            copy = remote(mine, part(kind, layer, col, img), xsend.at[t, d - 1], xrecv.at[t, d - 1], xpeer(d))
            copy.start()
            sends.append(copy)
        copy = remote(hbm[kind].at[layer], shard(kind, layer, col), psend.at[t], precv.at[t], partner)
        copy.start()
        sends.append(copy)
        pltpu.make_async_copy(hbm[kind].at[layer], shard(kind, layer, col), local_sem.at[t]).start()

    def owner_at(d, lane):
        return lax.rem(chip + chips - d, chips) * 2 + lane

    def forward_x(t):
        layer, kind = divmod(t, 4)
        for d in range(1, chips):
            got = part(kind, layer, owner_at(d, core), img)
            remote(got, got, xsend.at[t, d - 1], xrecv.at[t, d - 1], xpeer(d)).wait_recv()
            for copy in (
                remote(got, got, ysend.at[t, d - 1], yrecv.at[t, d - 1], ypeer),
                remote(got, got, fsend.at[t, d - 1, 0], frecv.at[t, d - 1, 0], partner),
            ):
                copy.start()
                sends.append(copy)

    def forward_y(t):
        layer, kind = divmod(t, 4)
        for d in range(1, chips):
            got = part(kind, layer, owner_at(d, core), 1 - img)
            remote(got, got, ysend.at[t, d - 1], yrecv.at[t, d - 1], ypeer).wait_recv()
            copy = remote(got, got, fsend.at[t, d - 1, 1], frecv.at[t, d - 1, 1], partner)
            copy.start()
            sends.append(copy)

    def ready(t):
        layer, kind = divmod(t, 4)
        pltpu.make_async_copy(hbm[kind].at[layer], shard(kind, layer, col), local_sem.at[t]).wait()
        other = shard(kind, layer, chip * 2 + (1 - core))
        remote(other, other, psend.at[t], precv.at[t], partner).wait_recv()
        for d in range(1, chips):
            for k, half in ((0, img), (1, 1 - img)):
                got = part(kind, layer, owner_at(d, 1 - core), half)
                remote(got, got, fsend.at[t, d - 1, k], frecv.at[t, d - 1, k], partner).wait_recv()

    def iota(shape, dim):
        return lax.broadcasted_iota(jnp.int32, shape, dim)

    wide = GROUP * AREA
    key = iota((AREA, wide), 0)
    query = iota((AREA, wide), 1) % AREA
    rowdiff[...] = ((key // (2 * PATCH)) != (query // (2 * PATCH))).astype(jnp.float32)
    coldiff[...] = (((key // PATCH) % 2) != ((query // PATCH) % 2)).astype(jnp.float32)
    pick = (key == query).astype(jnp.bfloat16)
    head_dim = channels // HEADS
    lanes = GROUP * head_dim
    own_head = iota((lanes, wide), 0) // head_dim == iota((lanes, wide), 1) // AREA
    head_masks = [(iota((AREA, lanes), 1) // head_dim == h).astype(jnp.bfloat16) for h in range(GROUP)]
    last_row = (row == n_row - 1).astype(jnp.float32)
    last_col = (col == n_col - 1).astype(jnp.float32)

    def base(half, patch_col):
        return (patch_col // 2) * AREA + half * 2 * PATCH + (patch_col % 2) * PATCH

    tok_copy.wait()
    tok32[...] = tok_ref[...].astype(jnp.float32)
    for r in range(WIN):
        for p in range(ncols):
            start = base(r // HALF, p) + (r % HALF) * HALF
            x32[start : start + HALF, :] = tok32[r, p * HALF : (p + 1) * HALF, :]

    span = 2 * WIN
    high = table_ref[...].astype(jnp.bfloat16)
    rest = table_ref[...] - high.astype(jnp.float32)
    middle = rest.astype(jnp.bfloat16)
    low = (rest - middle.astype(jnp.float32)).astype(jnp.bfloat16)
    thirds = jnp.concatenate([high, middle, low], axis=0)
    count = table_ref.shape[0]

    def positions(rb):
        slot = iota((table_ref.shape[1], wide), 0)
        lane = iota((table_ref.shape[1], wide), 1)
        at = lane % AREA
        ra = (at // (2 * PATCH)) * HALF + (at % PATCH) // HALF
        onehot = (slot == (lane // AREA) * span + ra - rb + WIN - 1).astype(jnp.bfloat16)
        found = jnp.dot(thirds, onehot, preferred_element_type=jnp.float32)
        found = found[:count] + found[count : 2 * count] + found[2 * count :]
        zrows[...] = found.reshape(zrows.shape)
        inner = iota((1, wide), 1) % AREA
        ca = ((inner // PATCH) % 2) * HALF + inner % HALF

        def one(n, carry):
            rows = jnp.zeros((WIN, wide), jnp.float32)
            for v in range(WIN):
                rows = jnp.where(ca == v, zrows[n, WIN - 1 - v : 2 * WIN - 1 - v, :], rows)
            groups = HEADS // GROUP
            for pc in range(2):
                first = (rb // HALF) * 2 * PATCH + pc * PATCH + (rb % HALF) * HALF
                pos_ref[n // groups, n % groups, first : first + HALF, :] = rows[pc * HALF : (pc + 1) * HALF]
            return carry

        lax.fori_loop(0, zrows.shape[0], one, 0)

    def position_range(rows):
        for rb in rows:
            positions(rb)

    def block(layer, targets, travel, stay, hooks):
        for w in range(nwin):
            rows = slice(w * AREA, (w + 1) * AREA)
            normed[rows, :] = layer_norm(
                x32[rows, :], gain_ref[layer, 0:1, :], mbias_ref[layer, 0:1, :]
            ).astype(jnp.bfloat16)
        hooks[0]()
        for c in range(3):
            cols = slice(c * channels, (c + 1) * channels)
            qkv_ref[:, cols] = (
                jnp.dot(normed[...], wqkv[layer, :, cols], preferred_element_type=jnp.float32)
                + qkvb_ref[layer : layer + 1, cols]
            ).astype(jnp.bfloat16)
        for w in range(nwin):
            hooks[1 + w]()
            rows = slice(w * AREA, (w + 1) * AREA)

            def one_group(g, carry):
                def lanes_of(which):
                    first = pl.multiple_of(which * channels + g * lanes, lanes)
                    return qkv_ref[rows, pl.ds(first, lanes)]

                q, k, v = lanes_of(0), lanes_of(1), lanes_of(2)
                stacked = jnp.concatenate([q * m for m in head_masks], axis=0)
                scores = lax.dot_general(
                    k, stacked, (((1,), (1,)), ((), ())), preferred_element_type=jnp.float32
                )
                scores = scores * (LOG2E / float(np.sqrt(head_dim))) + pos_ref[layer, g]
                if layer == 1:
                    differs = rowdiff[...] * last_row
                    if w == nwin - 1:
                        differs = differs + coldiff[...] * last_col
                    scores = jnp.where(differs > 0.0, -1000000000.0 * LOG2E, scores)
                top = jnp.max(scores, axis=0, keepdims=True)
                weight = jnp.exp2(scores - top)
                total = jnp.sum(weight, axis=0, keepdims=True)
                mixed = lax.dot_general(
                    v, weight.astype(jnp.bfloat16), (((0,), (0,)), ((), ())), preferred_element_type=jnp.float32
                )
                mixed = jnp.where(own_head, mixed * (1.0 / total), 0.0).astype(jnp.bfloat16)
                gathered = lax.dot_general(
                    pick, mixed, (((1,), (1,)), ((), ())), preferred_element_type=jnp.float32
                )
                heads_ref[rows, pl.ds(pl.multiple_of(g * lanes, lanes), lanes)] = gathered.astype(jnp.bfloat16)
                return carry

            lax.fori_loop(0, HEADS // GROUP, one_group, 0, unroll=4)
        hooks[1 + nwin]()
        y32[...] = x32[...] + (
            jnp.dot(heads_ref[...], wproj[layer], preferred_element_type=jnp.float32)
            + mbias_ref[layer, 2:3, :]
        )
        hooks[2 + nwin]()
        mlp(layer, [*travel[0], *travel[1], *travel[2]], hooks[3 + nwin])
        copies, at = [], 0
        for which, (source, landing) in enumerate(((sa, ra), (sb, rb), (sc, rc))):
            size = len(travel[which]) * PATCH
            source[layer] = m32[at : at + size, :].astype(jnp.bfloat16)
            at += size
            copy = remote(
                source.at[layer], landing.at[layer], hsend.at[layer, which], hrecv.at[layer, which], targets[which]
            )
            copy.start()
            copies.append(copy)
        mlp(layer, stay, nothing)
        return copies

    def mlp(layer, patches, before_output):
        rows = slice(0, -(-len(patches) * PATCH // 16) * 16)
        for at, (half, p) in enumerate(patches):
            first = base(half, p)
            m32[at * PATCH : (at + 1) * PATCH, :] = y32[first : first + PATCH, :]
        normed[rows, :] = layer_norm(
            m32[rows, :], gain_ref[layer, 1:2, :], mbias_ref[layer, 1:2, :]
        ).astype(jnp.bfloat16)
        chunk = 512
        for c in range(whid.shape[2] // chunk):
            cols = slice(c * chunk, (c + 1) * chunk)
            pre = (
                jnp.dot(normed[rows, :], whid[layer, :, cols], preferred_element_type=jnp.float32)
                + hidb_ref[layer : layer + 1, cols]
            )
            hidden_ref[rows, cols] = (0.5 * pre * (1.0 + lax.erf(pre * float(np.sqrt(0.5))))).astype(jnp.bfloat16)
        before_output()
        final = m32[rows, :] + (
            jnp.dot(hidden_ref[rows, :], wout[layer], preferred_element_type=jnp.float32)
            + mbias_ref[layer, 3:4, :]
        )
        m32[rows, :] = final.astype(jnp.bfloat16).astype(jnp.float32)

    def nothing():
        pass

    def steps(*calls):
        def run():
            for call, t in calls:
                call(t)

        return run

    m32[...] = jnp.zeros_like(m32)
    travel = ([(0, p) for p in range(1, ncols)], [(1, 0)], [(0, 0)])
    stay = [(1, p) for p in range(1, ncols)]
    copies = block(0, back, travel, stay, [
        steps(
            (position_range, range(0, 5)), (forward_x, 0), (position_range, range(5, 8)), (forward_x, 1),
            (position_range, range(8, WIN)), (forward_y, 0), (forward_x, 2), (ready, 0),
        ),
        steps((forward_y, 1)),
        nothing,
        steps((forward_x, 3), (forward_y, 2)),
        steps((ready, 1)),
        steps((forward_x, 4), (ready, 2)),
        steps((forward_y, 3), (forward_x, 5), (ready, 3)),
    ])
    for p in range(ncols - 1):
        at = base(0, p)
        x32[at : at + PATCH, :] = m32[p * PATCH : (p + 1) * PATCH, :]
    steps((forward_y, 4), (forward_x, 6), (forward_y, 5))()
    for copy in copies:
        copy.wait()
    stage[...] = ra[0].astype(jnp.float32)
    for p in range(ncols - 1):
        at = base(1, p)
        x32[at : at + PATCH, :] = stage[p * PATCH : (p + 1) * PATCH, :]
    at = base(0, ncols - 1)
    x32[at : at + PATCH, :] = rb[0].astype(jnp.float32)
    at = base(1, ncols - 1)
    x32[at : at + PATCH, :] = rc[0].astype(jnp.float32)

    travel = ([(1, p) for p in range(ncols - 1)], [(0, ncols - 1)], [(1, ncols - 1)])
    stay = [(0, p) for p in range(ncols - 1)]
    copies = block(1, forth, travel, stay, [
        steps((ready, 4), (forward_x, 7)),
        steps((forward_y, 6)),
        nothing,
        steps((forward_y, 7)),
        steps((ready, 5)),
        steps((ready, 6)),
        steps((ready, 7)),
    ])
    def put(source, start, half, p):
        for r in range(HALF):
            tok32[half * HALF + r, p * HALF : (p + 1) * HALF, :] = source[
                start + r * HALF : start + (r + 1) * HALF, :
            ]

    for p in range(ncols - 1):
        put(m32, p * PATCH, 1, p + 1)
    for copy in copies:
        copy.wait()
    stage[...] = ra[1].astype(jnp.float32)
    for p in range(ncols - 1):
        put(stage, p * PATCH, 0, p + 1)
    stage[0:PATCH, :] = rb[1].astype(jnp.float32)
    stage[PATCH : 2 * PATCH, :] = rc[1].astype(jnp.float32)
    put(stage, 0, 1, 0)
    put(stage, PATCH, 0, 0)
    out_ref[...] = tok32[...].astype(jnp.bfloat16)
    for copy in sends:
        copy.wait_send()


def local(sizes, tokens, qkv_w, proj_w, hid_w, out_w, gain, mbias, qkvb, hidb, position):
    table = position_rows(position)
    n_col, n_img = sizes[1], sizes[2]
    chips = n_col // 2
    height, width, channels = tokens.shape
    count = height * width
    f32, bf16 = jnp.float32, jnp.bfloat16
    hop = (width // HALF - 1) * PATCH
    dma = pltpu.SemaphoreType.DMA

    def full(w):
        return pltpu.VMEM((w.shape[0], w.shape[1] * n_col, w.shape[2]), bf16)

    any_spec = pl.BlockSpec(memory_space=pl.ANY)
    vmem_spec = pl.BlockSpec(memory_space=pltpu.VMEM)
    return pl.pallas_call(
        functools.partial(kernel, sizes),
        out_shape=jax.ShapeDtypeStruct(tokens.shape, bf16),
        in_specs=[any_spec] * 5 + [vmem_spec] * 5,
        out_specs=vmem_spec,
        scratch_shapes=[
            full(qkv_w), full(proj_w), full(hid_w), full(out_w),
            pltpu.VMEM((2, HEADS // GROUP, AREA, GROUP * AREA), f32),
            pltpu.VMEM(tokens.shape, bf16),
            pltpu.VMEM(tokens.shape, f32),
            pltpu.VMEM((count, channels), f32),
            pltpu.VMEM((count, channels), bf16),
            pltpu.VMEM((count, 3 * channels), bf16),
            pltpu.VMEM((count, channels), bf16),
            pltpu.VMEM((count, hid_w.shape[2]), bf16),
            pltpu.VMEM((count, channels), f32),
            pltpu.VMEM((-(-(hop + 2 * PATCH) // 16) * 16, channels), f32),
            pltpu.VMEM((hop, channels), f32),
            pltpu.VMEM((AREA, GROUP * AREA), f32),
            pltpu.VMEM((AREA, GROUP * AREA), f32),
            pltpu.VMEM((2 * HEADS // GROUP, 2 * WIN, GROUP * AREA), f32),
            pltpu.VMEM((2, hop, channels), bf16),
            pltpu.VMEM((2, PATCH, channels), bf16),
            pltpu.VMEM((2, PATCH, channels), bf16),
            pltpu.VMEM((2, hop, channels), bf16),
            pltpu.VMEM((2, PATCH, channels), bf16),
            pltpu.VMEM((2, PATCH, channels), bf16),
            dma((10,)),
            dma((8,)), dma((8,)),
            dma((8, chips - 1)), dma((8, chips - 1)),
            dma((8, chips - 1)), dma((8, chips - 1)),
            dma((8, chips - 1, 2)), dma((8, chips - 1, 2)),
            dma((2, 3)), dma((2, 3)),
        ],
        compiler_params=pltpu.CompilerParams(
            collective_id=0, has_side_effects=True, vmem_limit_bytes=62 * 1024 * 1024
        ),
        name="swin_pair",
    )(tokens, qkv_w, proj_w, hid_w, out_w, gain, mbias, qkvb, hidb, table)


def solution(mesh):
    in_specs = (P(("img", "row"), "col", None),) + (P(None, "col", None),) * 4 + (P(),) * 5
    sizes = tuple(mesh.shape[a] for a in ("row", "col", "img"))
    return jax.shard_map(
        functools.partial(local, sizes),
        mesh=mesh,
        in_specs=in_specs,
        out_specs=P(("img", "row"), "col", None),
        check_vma=False,
    )
```
